32 devices in a mesh: expert: 8 (over z, y), vocab: 4 (over x, core).
Axes of the slice: x: 2, y: 2, z: 4, core: 2. Of those that a mesh axis runs over, the one named last changes fastest.
Arguments:
- layer_out: bfloat16 [256, 2048], P('expert'), may hold values from -6 to 6
- moe_input: bfloat16 [256, 2048], P('expert'), may hold values from -6 to 6
- final_gain: float32 [2048], replicated, may hold values from 0.1 to 1.9
- head_weight: bfloat16 [2048, 12288], P(None, ('expert', 'vocab')), may hold values from -0.125 to 0.125
- clean_ids: int32 [256], P('expert'), may hold values from 0 to 12287
- levels: int32 [256], P('expert'), may hold values from 0 to 15
- ratio_table: float32 [16], replicated, may hold values from 0.5 to 8
- gate_weights: float32 [256, 8], P('expert'), may hold values from 0.05 to 0.5
- expert_ids: int32 [256, 8], P('expert'), may hold values from 0 to 15, all different within a row; in each aligned block of 32 rows (0 to 31, 32 to 63, ...) at most 32 rows name the same one
- w_gate: bfloat16 [16, 2048, 1024], P('expert', None, 'vocab'), may hold values from -0.125 to 0.125
- w_up: bfloat16 [16, 2048, 1024], P('expert', None, 'vocab'), may hold values from -0.125 to 0.125
- w_down: bfloat16 [16, 1024, 2048], P('expert', 'vocab'), may hold values from -0.1875 to 0.1875
Outputs:
- head_grad: float32 [2048, 12288], P(None, ('expert', 'vocab'))
- residual_grad: float32 [256, 2048], P('expert', 'vocab')
- input_grad: float32 [256, 2048], P('expert', 'vocab')
The draws below stay inside these ranges and needn't reach their ends.
Inputs may be any that keep to these rules, and one draw needn't show every extreme that they name: `expert_ids`: the 8 experts of a row are distinct; among the 32 rows of one index of expert no expert is named by more than 32 rows.
All inputs are finite; a program needn't handle non-finite values.
Results may differ from the reference program's by a relative error of at most 0.0044.
The reference program's roundings to bfloat16 on the way (of `normed`, `score_grad` and `routed_grad`) count: a program that leaves them out, or rounds other values in their place, can miss the bound.
Values may be sent and summed in bfloat16 or wider, within the bound.
A program may use at most 64 MiB of HBM per device.

```python
import math
import jax
import jax.numpy as jnp
import numpy as np
from jax import lax

D = 2048
FF = 1024
TOP = 8
VOC_DEV = 384
ROWS_DEV = 32
LEVELS = 16
EXPERTS = 16
VOCAB = 12288
ROWS = 256
CAP = 32
N_EXPERT = 8
N_VOCAB = 4


def with_ends(values, key, low, top_value):
    spot = [jax.random.randint(jax.random.fold_in(key, axis), (), 0, length) for axis, length in enumerate(values.shape)]
    widest = values.shape.index(max(values.shape))
    next_to = spot[:widest] + [(spot[widest] + 1) % values.shape[widest]] + spot[widest + 1:]
    return values.at[tuple(spot)].set(low).at[tuple(next_to)].set(top_value)


def block_levels(rng, shape, shards, smallest, top_value):
    gain, own = 1.0, jax.random.fold_in(rng, 6)
    for dim, parts in shards:
        draws = jnp.exp(jax.random.uniform(jax.random.fold_in(own, dim), (parts,), jnp.float32, smallest / len(shards), top_value / len(shards)))
        gain = gain * jnp.repeat(draws, shape[dim] // parts).reshape([-1 if axis == dim else 1 for axis in range(len(shape))])
    return gain


def cumulative_ranks(amount, slope):
    portions = [(1 << 20) // math.isqrt(standing ** slope) + 1 for standing in range(1, amount + 1)]
    scale = 1 + sum(portions) // (1 << 30)
    return np.cumsum(np.array([max(1, weight // scale) for weight in portions]))


def ranked(key, extent, count, skew):
    listing = cumulative_ranks(count, skew)
    ticket = jax.random.randint(jax.random.fold_in(key, 1), extent, 0, int(listing[count - 1]))
    rank = jnp.searchsorted(jnp.asarray(listing, jnp.int32), ticket, side="right")
    return jax.random.permutation(jax.random.fold_in(key, 2), count)[rank].astype(jnp.int32)


def assign_block(key, own, number, rows, amount, top, most, skew):
    sequence = jax.random.permutation(key, amount)
    packed, ordinary = shares(amount, rows * top, most, skew, True), shares(amount, rows * top, most, skew, False)
    places = jnp.arange(amount)

    def named(lengths, rotation):
        used = int((lengths > 0).sum())
        fixed = max(1, used // 4)
        shifted = fixed + (places - fixed + rotation * (used - fixed)) % max(1, amount - fixed)
        return jnp.zeros((amount,), jnp.int32).at[sequence[jnp.where(places < fixed, places, shifted)]].set(jnp.asarray(lengths, jnp.int32))

    lengths = jnp.where(number % 4 == 0, named(packed, number // 4), named(ordinary, number - number // 4 - 1))
    mixed = jax.random.permutation(jax.random.fold_in(own, 3), amount)
    donor, receiver = mixed[0:amount // 2 * 2:2], mixed[1:amount // 2 * 2:2]
    room = jnp.minimum(lengths[donor] - 1, most - lengths[receiver]) // 2
    room = jnp.where((donor == sequence[0]) | (receiver == sequence[0]) | (lengths[receiver] == 0), 0, jnp.maximum(room, 0))
    shifted = jax.random.randint(jax.random.fold_in(own, 4), (amount // 2,), 0, 1 << 20) % (room + 1)
    lengths = lengths.at[donor].add(-shifted).at[receiver].add(shifted)
    items = jnp.searchsorted(jnp.cumsum(lengths), jnp.arange(rows * top), side="right").astype(jnp.int32)
    listing = items.reshape(top, rows).T
    listing = listing[jax.random.permutation(jax.random.fold_in(own, 1), rows)]
    rotation = jax.random.randint(jax.random.fold_in(own, 2), (rows, 1), 0, top)
    return jnp.take_along_axis(listing, (jnp.arange(top)[None, :] + rotation) % top, axis=1)


def shares(count, total, reach, lean, full):
    loads = [(1 << 20) // math.isqrt(grade ** lean) + 1 for grade in range(1, count + 1)]
    largest = reach if full else min(reach, max(-(-total // count), total * loads[0] // sum(loads)))
    least = 1 if total - largest >= count - 1 else 0
    holding, surplus = [largest] + [least] * (count - 1), total - largest - least * (count - 1)
    while surplus > 0:
        free = [i for i in range(1, count) if holding[i] < largest] or [i for i in range(1, count) if holding[i] < reach]
        pool, budget = sum([loads[i] for i in free]), surplus
        for i in free:
            extra = min(reach - holding[i], max(1, budget * loads[i] // pool), surplus)
            holding[i] = holding[i] + extra
            surplus = surplus - extra
    return np.array(holding)


def noise(stream_key, shape, spread, limit, shards=(), kind=jnp.bfloat16):
    entries = jax.random.normal(stream_key, shape, jnp.float32) * spread
    if len(shards) > 0:
        entries = block_levels(stream_key, shape, shards, -0.22, 0.18) * entries
    return jnp.clip(entries, min=-limit, max=limit).astype(kind)


def setup_inputs(seed: int = 0) -> dict:
    streams_of = jax.random.split(jax.random.key(seed), 13)
    layer_out = noise(streams_of[0], (ROWS, D), 1.0, 6.0, ((0, 8),))
    moe_input = noise(streams_of[1], (ROWS, D), 1.0, 6.0, ((0, 8),))
    final_gain = jnp.clip(1.0 + 0.18 * jax.random.normal(streams_of[2], (D,), jnp.float32), 0.1, 1.9)
    head_weight = noise(streams_of[3], (D, VOCAB), D ** -0.5, 0.125, ((1, 32),))
    clean_ids = with_ends(ranked(streams_of[4], (ROWS,), VOCAB, 2), jax.random.fold_in(streams_of[4], 3), 0, VOCAB - 1).astype(jnp.int32)
    levels = with_ends(jax.random.randint(streams_of[5], (ROWS,), 0, LEVELS), jax.random.fold_in(streams_of[5], 1), 0, LEVELS - 1).astype(jnp.int32)
    ratio_table = jnp.clip(jnp.exp(jax.random.uniform(streams_of[6], (LEVELS,), jnp.float32, math.log(0.5), math.log(8.0))), 0.5, 8.0)
    gate_weights = jnp.clip(jnp.exp(math.log(0.5) - 2.3025851 * jax.random.uniform(streams_of[7], (ROWS, TOP), jnp.float32) ** block_levels(streams_of[7], (ROWS, TOP), ((0, 8),), -0.2, 0.2)), 0.05, 0.5)
    expert_ids_keys = jax.random.split(jax.random.fold_in(streams_of[8], 1), ROWS // ROWS_DEV)
    expert_ids_turns = jax.random.permutation(jax.random.fold_in(streams_of[8], 3), ROWS // ROWS_DEV)
    expert_ids = jax.vmap(lambda own, number: assign_block(jax.random.fold_in(streams_of[8], 2), own, number, ROWS_DEV, EXPERTS, TOP, CAP, 2))(expert_ids_keys, expert_ids_turns).reshape((ROWS, TOP))
    w_gate = noise(streams_of[9], (EXPERTS, D, FF), D ** -0.5, 0.125, ((0, 8), (2, 4)))
    w_up = noise(streams_of[10], (EXPERTS, D, FF), D ** -0.5, 0.125, ((0, 8), (2, 4)))
    w_down = noise(streams_of[11], (EXPERTS, FF, D), FF ** -0.5, 0.1875, ((0, 8), (1, 4)))
    return {"layer_out": layer_out, "moe_input": moe_input, "final_gain": final_gain, "head_weight": head_weight, "clean_ids": clean_ids, "levels": levels, "ratio_table": ratio_table, "gate_weights": gate_weights, "expert_ids": expert_ids, "w_gate": w_gate, "w_up": w_up, "w_down": w_down}


epsilon = 1e-05

def slot_positions(expert_ids):
    id_blocks = expert_ids.reshape(N_EXPERT, ROWS_DEV * TOP)
    labels = jnp.arange(EXPERTS, dtype=jnp.int32)
    onehot = (id_blocks[:, :, None] == labels[None, None, :]).astype(jnp.int32)
    earlier = jnp.cumsum(onehot, axis=1) - onehot
    slot_index = lax.optimization_barrier(jnp.sum(earlier * onehot, axis=2))
    source = jnp.arange(N_EXPERT, dtype=jnp.int32)[:, None]
    position = id_blocks * (N_EXPERT * CAP) + source * CAP + slot_index
    return position.reshape(-1).astype(jnp.int32)

def expert_backward(operands):
    inputs_slot, grads_slot, gate_matrix, up_matrix, down_matrix = operands
    inputs_wide = inputs_slot.astype(jnp.float32)
    gate_pre = jnp.dot(inputs_wide, gate_matrix.astype(jnp.float32), preferred_element_type=jnp.float32)
    up_pre = jnp.dot(inputs_wide, up_matrix.astype(jnp.float32), preferred_element_type=jnp.float32)
    act_grad = jnp.dot(grads_slot.astype(jnp.float32), down_matrix.astype(jnp.float32).T, preferred_element_type=jnp.float32)
    sigmoid_gate = jax.nn.sigmoid(gate_pre)
    gate_grad = (act_grad * up_pre * sigmoid_gate * (1.0 + gate_pre * (1.0 - sigmoid_gate))).astype(jnp.bfloat16)
    up_grad = (act_grad * gate_pre * sigmoid_gate).astype(jnp.bfloat16)
    first = jnp.dot(gate_grad.astype(jnp.float32), gate_matrix.astype(jnp.float32).T, preferred_element_type=jnp.float32)
    second = jnp.dot(up_grad.astype(jnp.float32), up_matrix.astype(jnp.float32).T, preferred_element_type=jnp.float32)
    return first + second

def reference(layer_out, moe_input, final_gain, head_weight, clean_ids, levels, ratio_table, gate_weights, expert_ids, w_gate, w_up, w_down):
    values = layer_out.astype(jnp.float32)
    row_scale = jnp.sqrt(lax.optimization_barrier(jnp.mean(values * values, axis=1, keepdims=True)) + epsilon)
    unit_rows = values / row_scale
    normed = (unit_rows * final_gain[None, :]).astype(jnp.bfloat16)
    normed_wide = normed.astype(jnp.float32)
    ratio_rows = ratio_table[levels]
    loss_scale = 1.0 / math.sqrt(ROWS)
    block_count = N_EXPERT * N_VOCAB
    weight_blocks = head_weight.reshape(D, block_count, VOC_DEV).transpose(1, 0, 2)

    def scan_step(accumulated, block_input):
        weight_block, block_index = block_input
        weight_wide = weight_block.astype(jnp.float32)
        scores = jnp.dot(normed_wide, weight_wide, preferred_element_type=jnp.float32)
        columns = block_index * VOC_DEV + jnp.arange(VOC_DEV, dtype=jnp.int32)
        target_hit = (clean_ids[:, None] == columns[None, :]).astype(jnp.float32)
        score_grad = ((jnp.exp(scores) - ratio_rows[:, None] * target_hit) * loss_scale).astype(jnp.bfloat16)
        grad_wide = score_grad.astype(jnp.float32)
        block_grad = jnp.dot(normed_wide.T, grad_wide, preferred_element_type=jnp.float32)
        accumulated = accumulated + jnp.dot(grad_wide, weight_wide.T, preferred_element_type=jnp.float32)
        return (accumulated, block_grad)
    normed_grad, grad_blocks = lax.scan(scan_step, jnp.zeros((ROWS, D), jnp.float32), (weight_blocks, jnp.arange(block_count, dtype=jnp.int32)))
    head_grad = grad_blocks.transpose(1, 0, 2).reshape(D, VOCAB)
    gained = final_gain[None, :] * normed_grad
    residual_grad = (gained - unit_rows * lax.optimization_barrier(jnp.mean(unit_rows * gained, axis=1, keepdims=True))) / row_scale
    routed_grad = (gate_weights[:, :, None] * residual_grad[:, None, :]).astype(jnp.bfloat16).reshape(ROWS * TOP, D)
    inputs_rep = jnp.repeat(moe_input, TOP, axis=0)
    position = slot_positions(expert_ids)
    buffer_rows = EXPERTS * N_EXPERT * CAP
    inputs_buffer = jnp.zeros((buffer_rows, D), jnp.bfloat16).at[position].set(inputs_rep)
    grads_buffer = jnp.zeros((buffer_rows, D), jnp.bfloat16).at[position].set(routed_grad)
    slot_grads = lax.map(expert_backward, (inputs_buffer.reshape(EXPERTS, N_EXPERT * CAP, D), grads_buffer.reshape(EXPERTS, N_EXPERT * CAP, D), w_gate, w_up, w_down))
    per_pair = slot_grads.reshape(buffer_rows, D)[position]
    input_grad = lax.optimization_barrier(jnp.sum(per_pair.reshape(ROWS, TOP, D), axis=1))
    return (head_grad, residual_grad, input_grad)
```

```python
import functools
import math

import jax
import jax.numpy as jnp
from jax import lax
from jax.experimental import pallas as pl
from jax.experimental.pallas import tpu as pltpu
from jax.sharding import PartitionSpec as P

epsilon = 1e-05
CORES = 2
MESH = pl.DeviceIdType.MESH
VMEM = pl.BlockSpec(memory_space=pltpu.VMEM)


def place():
    e, v = lax.axis_index("expert"), lax.axis_index("vocab")
    n_expert, n_vocab = lax.axis_size("expert"), lax.axis_size("vocab")
    return e, v // CORES, v % CORES, n_expert, n_vocab // CORES


def device(e, a, c):
    return (e, a * CORES + c)


def greet(devices):
    barrier = pltpu.get_barrier_semaphore()
    for other in devices:
        pl.semaphore_signal(barrier, inc=1, device_id=other, device_id_type=MESH)
    pl.semaphore_wait(barrier, len(devices))


def remote(src, dst, send, recv, target):
    return pltpu.make_async_remote_copy(
        src_ref=src, dst_ref=dst, send_sem=send, recv_sem=recv, device_id=target,
        device_id_type=MESH,
    )


def gather_kernel(n_data, n_meta, *refs):
    count = n_data + n_meta
    ins, outs = refs[:count], refs[count:2 * count]
    local_sem, e_send, e_recv, a_send, a_recv, c_send, c_recv, m_send, m_recv = refs[2 * count:]
    e, a, c, n_e, n_a = place()
    expert_peer = [device(lax.rem(e + d, n_e), a, c) for d in range(1, n_e)]
    chip_peer = [device(e, lax.rem(a + d, n_a), c) for d in range(1, n_a)]
    sibling = device(e, a, 1 - c)
    greet(expert_peer + chip_peer + [sibling])
    share = ins[0].shape[1]

    def block(i, eb, ab, cb):
        start = pl.multiple_of((ab * CORES + cb) * share, share)
        return outs[i].at[eb, :, pl.ds(start, share)]

    sends = []

    def start(*args):
        copy = remote(*args)
        copy.start()
        sends.append(copy)

    locals_ = []
    for m in range(n_meta):
        i = n_data + m
        for d in range(1, n_e):
            start(ins[i], outs[i].at[e], m_send.at[m, d], m_recv.at[m, d], expert_peer[d - 1])
        own = pltpu.make_async_copy(ins[i], outs[i].at[e], local_sem.at[i])
        own.start()
        locals_.append(own)
    for i in range(n_data):
        for d in range(1, n_e):
            start(ins[i], block(i, e, a, c), e_send.at[i, d], e_recv.at[i, d], expert_peer[d - 1])
        own = pltpu.make_async_copy(ins[i], block(i, e, a, c), local_sem.at[i])
        own.start()
        locals_.append(own)
    for i in range(n_data):
        for d in range(n_e):
            eb = lax.rem(e + n_e - d, n_e)
            mine = block(i, eb, a, c)
            if d:
                remote(mine, mine, e_send.at[i, d], e_recv.at[i, d], sibling).wait_recv()
            src = mine if d else ins[i]
            for da in range(1, n_a):
                start(src, mine, a_send.at[i, d, da], a_recv.at[i, d, da], chip_peer[da - 1])
            start(src, mine, c_send.at[i, d, 0], c_recv.at[i, d, 0], sibling)
    for i in range(n_data):
        for d in range(n_e):
            eb = lax.rem(e + n_e - d, n_e)
            for da in range(1, n_a):
                other = block(i, eb, lax.rem(a + n_a - da, n_a), c)
                remote(other, other, a_send.at[i, d, da], a_recv.at[i, d, da], sibling).wait_recv()
                start(other, other, c_send.at[i, d, da], c_recv.at[i, d, da], sibling)
    for own in locals_:
        own.wait()
    for m in range(n_meta):
        for d in range(1, n_e):
            slot = outs[n_data + m].at[lax.rem(e + n_e - d, n_e)]
            remote(slot, slot, m_send.at[m, d], m_recv.at[m, d], sibling).wait_recv()
    for i in range(n_data):
        for d in range(n_e):
            eb = lax.rem(e + n_e - d, n_e)
            for da in range(n_a):
                other = block(i, eb, lax.rem(a + n_a - da, n_a), 1 - c)
                remote(other, other, c_send.at[i, d, da], c_recv.at[i, d, da], sibling).wait_recv()
    for copy in sends:
        copy.wait_send()


def gather_all(data, meta, collective_id):
    n_e, n_a = lax.axis_size("expert"), lax.axis_size("vocab") // CORES
    n_data, n_meta = len(data), len(meta)
    width = data[0].shape[1] * n_a * CORES
    out_shape = [jax.ShapeDtypeStruct((n_e, x.shape[0], width), x.dtype) for x in data]
    out_shape += [jax.ShapeDtypeStruct((n_e, *x.shape), x.dtype) for x in meta]
    dma = pltpu.SemaphoreType.DMA
    more = max(n_meta, 1)
    outs = pl.pallas_call(
        functools.partial(gather_kernel, n_data, n_meta),
        out_shape=out_shape,
        in_specs=[VMEM] * (n_data + n_meta),
        out_specs=[VMEM] * (n_data + n_meta),
        scratch_shapes=[
            dma((n_data + n_meta,)),
            dma((n_data, n_e)), dma((n_data, n_e)),
            dma((n_data, n_e, n_a)), dma((n_data, n_e, n_a)),
            dma((n_data, n_e, n_a)), dma((n_data, n_e, n_a)),
            dma((more, n_e)), dma((more, n_e)),
        ],
        compiler_params=pltpu.CompilerParams(collective_id=collective_id, has_side_effects=True),
    )(*data, *meta)
    return [x.reshape(-1, x.shape[-1]) for x in outs]


def core_kernel(x_ref, y_ref, send, recv):
    e, a, c, _, n_a = place()
    sibling = device(e, a, 1 - c)
    greet([sibling])
    share = y_ref.shape[2]
    copies = []
    for k in range(n_a):
        start = pl.multiple_of((k * CORES + 1 - c) * share, share)
        copy = remote(x_ref.at[:, pl.ds(start, share)], y_ref.at[k], send.at[k], recv.at[k], sibling)
        copy.start()
        copies.append(copy)
    for copy in copies:
        copy.wait()


def core_swap(x, collective_id):
    n_a = lax.axis_size("vocab") // CORES
    share = x.shape[1] // (n_a * CORES)
    dma = pltpu.SemaphoreType.DMA
    return pl.pallas_call(
        core_kernel,
        out_shape=jax.ShapeDtypeStruct((n_a, x.shape[0], share), x.dtype),
        in_specs=[VMEM],
        out_specs=VMEM,
        scratch_shapes=[dma((n_a,)), dma((n_a,))],
        compiler_params=pltpu.CompilerParams(collective_id=collective_id, has_side_effects=True),
    )(x)


def swap_kernel(kind, n, x_ref, y_ref, send, recv):
    e, a, c, _, _ = place()
    me = {"expert": e, "chip": a, "vocab": a * CORES + c}[kind]
    others = [lax.rem(me + d, n) for d in range(1, n)]

    def at(p):
        if kind == "expert":
            return device(p, a, c)
        return device(e, p, c) if kind == "chip" else (e, p)

    greet([at(p) for p in others])
    copies = []
    for d, p in enumerate(others):
        src = x_ref if kind == "vocab" else x_ref.at[p]
        copy = remote(src, y_ref.at[d], send.at[d], recv.at[d], at(p))
        copy.start()
        copies.append(copy)
    for copy in copies:
        copy.wait()


def swap(x, kind, n, collective_id):
    block = x.shape if kind == "vocab" else x.shape[1:]
    dma = pltpu.SemaphoreType.DMA
    return pl.pallas_call(
        functools.partial(swap_kernel, kind, n),
        out_shape=jax.ShapeDtypeStruct((n - 1, *block), x.dtype),
        in_specs=[VMEM],
        out_specs=VMEM,
        scratch_shapes=[dma((n - 1,)), dma((n - 1,))],
        compiler_params=pltpu.CompilerParams(collective_id=collective_id, has_side_effects=True),
    )(x)


def scatter_sum(partial, chip_type, expert_type, first_id):
    e, a, c, n_e, n_a = place()
    rows, width = partial.shape
    share = width // (n_a * CORES)
    other = core_swap(partial, first_id)
    by_chip = jnp.stack([
        lax.dynamic_slice_in_dim(partial, (k * CORES + c) * share, share, 1) + other[k]
        for k in range(n_a)
    ])
    arrived = swap(by_chip.astype(chip_type), "chip", n_a, first_id + 1)
    total = lax.dynamic_index_in_dim(by_chip, a, 0, False)
    total = total + jnp.sum(arrived.astype(jnp.float32), axis=0)
    by_row = total.reshape(n_e, rows // n_e, share)
    arrived = swap(by_row.astype(expert_type), "expert", n_e, first_id + 2)
    own = lax.dynamic_index_in_dim(by_row, e, 0, False)
    return own + jnp.sum(arrived.astype(jnp.float32), axis=0)


def on_device(
    layer_out,
    moe_input,
    final_gain,
    head_weight,
    clean_ids,
    levels,
    ratio_table,
    gate_weights,
    expert_ids,
    w_gate,
    w_up,
    w_down,
):
    rows_local, model_width = layer_out.shape
    n_expert = lax.axis_size("expert")
    n_vocab = lax.axis_size("vocab")
    expert_at, vocab_at = lax.axis_index("expert"), lax.axis_index("vocab")
    total_rows = rows_local * n_expert
    local_experts = w_gate.shape[0]
    experts_all = local_experts * n_expert
    share = model_width // n_vocab
    vocab_local = head_weight.shape[1]

    def own_share(x, axis):
        return lax.dynamic_slice_in_dim(x, vocab_at * share, share, axis)

    values = layer_out.astype(jnp.float32)
    row_scale = jnp.sqrt(jnp.mean(values * values, axis=1, keepdims=True) + epsilon)
    unit_share = own_share(layer_out, 1).astype(jnp.float32) / row_scale
    gain_share = own_share(final_gain, 0)[None, :]
    normed_share = (unit_share * gain_share).astype(jnp.bfloat16)
    labels = jnp.arange(experts_all, dtype=jnp.int32)
    gates = jnp.sum(
        jnp.where(expert_ids[:, :, None] == labels, gate_weights[:, :, None], 0.0), axis=1
    )
    level_labels = jnp.arange(ratio_table.shape[0], dtype=jnp.int32)
    ratio_rows = jnp.sum(
        jnp.where(levels[:, None] == level_labels[None, :], ratio_table[None, :], 0.0),
        axis=1, keepdims=True,
    )
    meta = jnp.concatenate([gates, ratio_rows, clean_ids[:, None].astype(jnp.float32)], axis=1)
    meta = jnp.pad(meta, ((0, 0), (0, -meta.shape[1] % 128)))
    normed_all, input_all, meta_all = gather_all(
        [normed_share, own_share(moe_input, 1)], [meta], 0
    )
    ratio_all = meta_all[:, experts_all:experts_all + 1]
    clean_all = meta_all[:, experts_all + 1:experts_all + 2].astype(jnp.int32)
    gate_all = lax.dynamic_slice_in_dim(meta_all, expert_at * local_experts, local_experts, 1)

    column_start = (expert_at * n_vocab + vocab_at) * vocab_local
    columns = column_start + jnp.arange(vocab_local, dtype=jnp.int32)
    scores = jnp.dot(normed_all, head_weight, preferred_element_type=jnp.float32)
    target_hit = (clean_all == columns[None, :]).astype(jnp.float32)
    loss_scale = 1.0 / math.sqrt(total_rows)
    score_grad = ((jnp.exp(scores) - ratio_all * target_hit) * loss_scale).astype(jnp.bfloat16)
    head_grad = lax.dot_general(
        normed_all, score_grad, (((0,), (0,)), ((), ())), preferred_element_type=jnp.float32
    )
    partial_grad = lax.dot_general(
        score_grad, head_weight, (((1,), (1,)), ((), ())), preferred_element_type=jnp.float32
    )
    normed_grad = scatter_sum(partial_grad, jnp.bfloat16, jnp.bfloat16, 1)
    gained = gain_share * normed_grad
    mean_part = jnp.sum(unit_share * gained, axis=1, keepdims=True) / model_width
    mean_part = jnp.broadcast_to(mean_part, (rows_local, 128))
    mean_row = mean_part + jnp.sum(swap(mean_part, "vocab", n_vocab, 4), axis=0)
    residual_grad = (gained - unit_share * mean_row[:, :1]) / row_scale
    (residual_all,) = gather_all([residual_grad.astype(jnp.bfloat16)], [], 5)

    partial_input = None
    for i in range(local_experts):
        gate_pre = jnp.dot(input_all, w_gate[i], preferred_element_type=jnp.float32)
        up_pre = jnp.dot(input_all, w_up[i], preferred_element_type=jnp.float32)
        act_grad = gate_all[:, i:i + 1] * lax.dot_general(
            residual_all, w_down[i], (((1,), (1,)), ((), ())), preferred_element_type=jnp.float32
        )
        s = jax.nn.sigmoid(gate_pre)
        gate_grad = (act_grad * up_pre * s * (1.0 + gate_pre * (1.0 - s))).astype(jnp.bfloat16)
        up_grad = (act_grad * gate_pre * s).astype(jnp.bfloat16)
        for grad, weight in ((gate_grad, w_gate[i]), (up_grad, w_up[i])):
            term = lax.dot_general(
                grad, weight, (((1,), (1,)), ((), ())), preferred_element_type=jnp.float32
            )
            partial_input = term if partial_input is None else partial_input + term
    input_grad = scatter_sum(partial_input, jnp.float32, jnp.bfloat16, 6)
    return (head_grad, residual_grad, input_grad)


def solution(mesh):
    in_specs = (
        P("expert", None),
        P("expert", None),
        P(),
        P(None, ("expert", "vocab")),
        P("expert"),
        P("expert"),
        P(),
        P("expert", None),
        P("expert", None),
        P("expert", None, "vocab"),
        P("expert", None, "vocab"),
        P("expert", "vocab", None),
    )
    out_specs = (P(None, ("expert", "vocab")), P("expert", "vocab"), P("expert", "vocab"))
    return jax.shard_map(
        on_device, mesh=mesh, in_specs=in_specs, out_specs=out_specs, check_vma=False
    )
```

```python
import functools
import math

import jax
import jax.numpy as jnp
from jax import lax
from jax.experimental import pallas as pl
from jax.experimental.pallas import tpu as pltpu
from jax.sharding import PartitionSpec as P

epsilon = 1e-05
CORES = 2
PAIR = 2
MESH = pl.DeviceIdType.MESH
VMEM = pl.BlockSpec(memory_space=pltpu.VMEM)


def place():
    e, v = lax.axis_index("expert"), lax.axis_index("vocab")
    n_expert, n_vocab = lax.axis_size("expert"), lax.axis_size("vocab")
    return e, v // CORES, v % CORES, n_expert, n_vocab // CORES


def device(e, a, c):
    return (e, a * CORES + c)


def greet(devices):
    barrier = pltpu.get_barrier_semaphore()
    for other in devices:
        pl.semaphore_signal(barrier, inc=1, device_id=other, device_id_type=MESH)
    pl.semaphore_wait(barrier, len(devices))


def remote(src, dst, send, recv, target):
    return pltpu.make_async_remote_copy(
        src_ref=src, dst_ref=dst, send_sem=send, recv_sem=recv, device_id=target,
        device_id_type=MESH,
    )


def gather_kernel(n_data, n_meta, *refs):
    count = n_data + n_meta
    ins, outs = refs[:count], refs[count:2 * count]
    local_sem, e_send, e_recv, a_send, a_recv, c_send, c_recv, m_send, m_recv = refs[2 * count:]
    e, a, c, n_e, n_a = place()
    n_o = n_e // PAIR
    o, inner = e // PAIR, e % PAIR
    outer_peer = [device(lax.rem(o + d, n_o) * PAIR + inner, a, c) for d in range(1, n_o)]
    inner_peer = device(o * PAIR + 1 - inner, a, c)
    chip_peer = [device(e, lax.rem(a + d, n_a), c) for d in range(1, n_a)]
    sibling = device(e, a, 1 - c)
    greet(outer_peer + [inner_peer] + chip_peer + [sibling])
    share = ins[0].shape[1]

    def source(b):
        across, d = b // n_o, b % n_o
        return lax.rem(o + n_o - d, n_o) * PAIR + (1 - inner if across else inner)

    def block(i, b, ab, cb):
        start = pl.multiple_of((ab * CORES + cb) * share, share)
        return outs[i].at[source(b), :, pl.ds(start, share)]

    sends, locals_ = [], []

    def start(*args):
        copy = remote(*args)
        copy.start()
        sends.append(copy)

    def landed(ref, recv):
        remote(ref, ref, recv, recv, sibling).wait_recv()

    for m in range(n_meta):
        for d in range(1, n_o):
            start(ins[n_data + m], outs[n_data + m].at[e], m_send.at[m, d], m_recv.at[m, d],
                  outer_peer[d - 1])
    for i in range(count):
        slot = block(i, 0, a, c) if i < n_data else outs[i].at[e]
        if i < n_data:
            for d in range(1, n_o):
                start(ins[i], slot, e_send.at[i, d], e_recv.at[i, d], outer_peer[d - 1])
        own = pltpu.make_async_copy(ins[i], slot, local_sem.at[i])
        own.start()
        locals_.append(own)
    for m in range(n_meta):
        for d in range(n_o):
            slot = outs[n_data + m].at[source(d)]
            if d:
                landed(slot, m_recv.at[m, d])
            start(slot if d else ins[n_data + m], slot, m_send.at[m, n_o + d],
                  m_recv.at[m, n_o + d], inner_peer)
    for i in range(n_data):
        for b in range(n_e):
            mine = block(i, b, a, c)
            if b:
                landed(mine, e_recv.at[i, b])
            src = mine if b else ins[i]
            if b < n_o:
                start(src, mine, e_send.at[i, n_o + b], e_recv.at[i, n_o + b], inner_peer)
            for da in range(1, n_a):
                start(src, mine, a_send.at[i, b, da], a_recv.at[i, b, da], chip_peer[da - 1])
            start(src, mine, c_send.at[i, b, 0], c_recv.at[i, b, 0], sibling)
    for i in range(n_data):
        for b in range(n_e):
            for da in range(1, n_a):
                other = block(i, b, lax.rem(a + n_a - da, n_a), c)
                landed(other, a_recv.at[i, b, da])
                start(other, other, c_send.at[i, b, da], c_recv.at[i, b, da], sibling)
    for own in locals_:
        own.wait()
    for m in range(n_meta):
        for d in range(n_o):
            landed(outs[n_data + m].at[source(n_o + d)], m_recv.at[m, n_o + d])
    for i in range(n_data):
        for b in range(n_e):
            for da in range(n_a):
                landed(block(i, b, lax.rem(a + n_a - da, n_a), 1 - c), c_recv.at[i, b, da])
    for copy in sends:
        copy.wait_send()


def gather_all(data, meta, collective_id):
    n_e, n_a = lax.axis_size("expert"), lax.axis_size("vocab") // CORES
    n_data, n_meta = len(data), len(meta)
    width = data[0].shape[1] * n_a * CORES
    out_shape = [jax.ShapeDtypeStruct((n_e, x.shape[0], width), x.dtype) for x in data]
    out_shape += [jax.ShapeDtypeStruct((n_e, *x.shape), x.dtype) for x in meta]
    dma = pltpu.SemaphoreType.DMA
    more = max(n_meta, 1)
    outs = pl.pallas_call(
        functools.partial(gather_kernel, n_data, n_meta),
        out_shape=out_shape,
        in_specs=[VMEM] * (n_data + n_meta),
        out_specs=[VMEM] * (n_data + n_meta),
        scratch_shapes=[
            dma((n_data + n_meta,)),
            dma((n_data, n_e)), dma((n_data, n_e)),
            dma((n_data, n_e, n_a)), dma((n_data, n_e, n_a)),
            dma((n_data, n_e, n_a)), dma((n_data, n_e, n_a)),
            dma((more, n_e)), dma((more, n_e)),
        ],
        compiler_params=pltpu.CompilerParams(collective_id=collective_id, has_side_effects=True),
    )(*data, *meta)
    return [x.reshape(-1, x.shape[-1]) for x in outs]


def swap_kernel(kind, n, x_ref, y_ref, send, recv):
    e, a, c, _, _ = place()
    me = {"expert": e, "chip": a, "vocab": a * CORES + c}[kind]
    others = [lax.rem(me + d, n) for d in range(1, n)]

    def at(p):
        if kind == "expert":
            return device(p, a, c)
        return device(e, p, c) if kind == "chip" else (e, p)

    greet([at(p) for p in others])
    copies = []
    for d, p in enumerate(others):
        src = x_ref if kind == "vocab" else x_ref.at[p]
        copy = remote(src, y_ref.at[d], send.at[d], recv.at[d], at(p))
        copy.start()
        copies.append(copy)
    for copy in copies:
        copy.wait()


def swap(x, kind, n, collective_id):
    block = x.shape if kind == "vocab" else x.shape[1:]
    dma = pltpu.SemaphoreType.DMA
    return pl.pallas_call(
        functools.partial(swap_kernel, kind, n),
        out_shape=jax.ShapeDtypeStruct((n - 1, *block), x.dtype),
        in_specs=[VMEM],
        out_specs=VMEM,
        scratch_shapes=[dma((n - 1,)), dma((n - 1,))],
        compiler_params=pltpu.CompilerParams(collective_id=collective_id, has_side_effects=True),
    )(x)


def scatter_kernel(x_ref, y_ref, from_core, to_chip, from_chip, own, to_row, from_row,
                   core_send, core_recv, chip_send, chip_recv, row_send, row_recv):
    e, a, c, n_e, n_a = place()
    rows, share = y_ref.shape
    sibling = device(e, a, 1 - c)
    chip_at = [lax.rem(a + d, n_a) for d in range(n_a)]
    row_at = [lax.rem(e + d, n_e) for d in range(n_e)]
    greet([sibling] + [device(e, p, c) for p in chip_at[1:]]
          + [device(p, a, c) for p in row_at[1:]])
    order = list(range(1, n_e)) + [0]
    sends = []

    def piece(s, k, cb):
        row = pl.multiple_of(row_at[s] * rows, rows)
        column = pl.multiple_of((chip_at[k] * CORES + cb) * share, share)
        return pl.ds(row, rows), pl.ds(column, share)

    def core_copy(s, k):
        return remote(x_ref.at[piece(s, k, 1 - c)], from_core.at[s, k], core_send.at[s, k],
                      core_recv.at[s, k], sibling)

    def chip_copy(s, k):
        return remote(to_chip.at[s, k], from_chip.at[s, k], chip_send.at[s, k],
                      chip_recv.at[s, k], device(e, chip_at[k], c))

    def row_copy(s):
        return remote(to_row.at[s], from_row.at[s], row_send.at[s], row_recv.at[s],
                      device(row_at[s], a, c))

    def start(copy):
        copy.start()
        sends.append(copy)

    turns = list(range(1, n_a)) + [0]
    for s in order:
        for k in turns:
            start(core_copy(s, k))

    def first(s):
        for k in turns:
            core_copy(s, k).wait_recv()
            term = x_ref[piece(s, k, c)] + from_core[s, k]
            if k:
                to_chip[s, k] = term.astype(to_chip.dtype)
                start(chip_copy(s, k))
            else:
                own[s] = term

    def second(s):
        term = own[s]
        for k in range(1, n_a):
            chip_copy(s, k).wait_recv()
            term = term + from_chip[s, k].astype(jnp.float32)
        if s:
            to_row[s] = term.astype(to_row.dtype)
            start(row_copy(s))
        else:
            y_ref[...] = term

    lag = 2
    for step in range(n_e + lag):
        if step < n_e:
            first(order[step])
        if step >= lag:
            second(order[step - lag])
    for s in range(1, n_e):
        row_copy(s).wait_recv()
        y_ref[...] += from_row[s].astype(jnp.float32)
    for copy in sends:
        copy.wait_send()


def scatter_sum(partial, chip_type, row_type, collective_id):
    n_e, n_a = lax.axis_size("expert"), lax.axis_size("vocab") // CORES
    rows, share = partial.shape[0] // n_e, partial.shape[1] // (n_a * CORES)
    dma = pltpu.SemaphoreType.DMA
    return pl.pallas_call(
        scatter_kernel,
        out_shape=jax.ShapeDtypeStruct((rows, share), jnp.float32),
        in_specs=[VMEM],
        out_specs=VMEM,
        scratch_shapes=[
            pltpu.VMEM((n_e, n_a, rows, share), jnp.float32),
            pltpu.VMEM((n_e, n_a, rows, share), chip_type),
            pltpu.VMEM((n_e, n_a, rows, share), chip_type),
            pltpu.VMEM((n_e, rows, share), jnp.float32),
            pltpu.VMEM((n_e, rows, share), row_type),
            pltpu.VMEM((n_e, rows, share), row_type),
            dma((n_e, n_a)), dma((n_e, n_a)), dma((n_e, n_a)), dma((n_e, n_a)),
            dma((n_e,)), dma((n_e,)),
        ],
        compiler_params=pltpu.CompilerParams(collective_id=collective_id, has_side_effects=True),
    )(partial)


def on_device(
    layer_out,
    moe_input,
    final_gain,
    head_weight,
    clean_ids,
    levels,
    ratio_table,
    gate_weights,
    expert_ids,
    w_gate,
    w_up,
    w_down,
):
    rows_local, model_width = layer_out.shape
    n_expert = lax.axis_size("expert")
    n_vocab = lax.axis_size("vocab")
    expert_at, vocab_at = lax.axis_index("expert"), lax.axis_index("vocab")
    total_rows = rows_local * n_expert
    local_experts = w_gate.shape[0]
    experts_all = local_experts * n_expert
    share = model_width // n_vocab
    vocab_local = head_weight.shape[1]

    def own_share(x, axis):
        return lax.dynamic_slice_in_dim(x, vocab_at * share, share, axis)

    values = layer_out.astype(jnp.float32)
    row_scale = jnp.sqrt(jnp.mean(values * values, axis=1, keepdims=True) + epsilon)
    unit_share = own_share(layer_out, 1).astype(jnp.float32) / row_scale
    gain_share = own_share(final_gain, 0)[None, :]
    normed_share = (unit_share * gain_share).astype(jnp.bfloat16)
    labels = jnp.arange(experts_all, dtype=jnp.int32)
    gates = jnp.sum(
        jnp.where(expert_ids[:, :, None] == labels, gate_weights[:, :, None], 0.0), axis=1
    )
    level_labels = jnp.arange(ratio_table.shape[0], dtype=jnp.int32)
    ratio_rows = jnp.sum(
        jnp.where(levels[:, None] == level_labels[None, :], ratio_table[None, :], 0.0),
        axis=1, keepdims=True,
    )
    meta = jnp.concatenate([gates, ratio_rows, clean_ids[:, None].astype(jnp.float32)], axis=1)
    meta = jnp.pad(meta, ((0, 0), (0, -meta.shape[1] % 128)))
    normed_all, input_all, meta_all = gather_all(
        [normed_share, own_share(moe_input, 1)], [meta], 0
    )
    ratio_all = meta_all[:, experts_all:experts_all + 1]
    clean_all = meta_all[:, experts_all + 1:experts_all + 2].astype(jnp.int32)
    gate_all = lax.dynamic_slice_in_dim(meta_all, expert_at * local_experts, local_experts, 1)

    column_start = (expert_at * n_vocab + vocab_at) * vocab_local
    columns = column_start + jnp.arange(vocab_local, dtype=jnp.int32)
    scores = jnp.dot(normed_all, head_weight, preferred_element_type=jnp.float32)
    target_hit = (clean_all == columns[None, :]).astype(jnp.float32)
    loss_scale = 1.0 / math.sqrt(total_rows)
    score_grad = ((jnp.exp(scores) - ratio_all * target_hit) * loss_scale).astype(jnp.bfloat16)
    head_grad = lax.dot_general(
        normed_all, score_grad, (((0,), (0,)), ((), ())), preferred_element_type=jnp.float32
    )
    partial_grad = lax.dot_general(
        score_grad, head_weight, (((1,), (1,)), ((), ())), preferred_element_type=jnp.float32
    )
    normed_grad = scatter_sum(partial_grad, jnp.float32, jnp.bfloat16, 1)
    gained = gain_share * normed_grad
    mean_part = jnp.sum(unit_share * gained, axis=1, keepdims=True) / model_width
    mean_part = jnp.broadcast_to(mean_part, (rows_local, 128))
    mean_row = mean_part + jnp.sum(swap(mean_part, "vocab", n_vocab, 4), axis=0)
    residual_grad = (gained - unit_share * mean_row[:, :1]) / row_scale
    (residual_all,) = gather_all([residual_grad.astype(jnp.bfloat16)], [], 5)

    partial_input = None
    for i in range(local_experts):
        gate_pre = jnp.dot(input_all, w_gate[i], preferred_element_type=jnp.float32)
        up_pre = jnp.dot(input_all, w_up[i], preferred_element_type=jnp.float32)
        act_grad = gate_all[:, i:i + 1] * lax.dot_general(
            residual_all, w_down[i], (((1,), (1,)), ((), ())), preferred_element_type=jnp.float32
        )
        s = jax.nn.sigmoid(gate_pre)
        gate_grad = (act_grad * up_pre * s * (1.0 + gate_pre * (1.0 - s))).astype(jnp.bfloat16)
        up_grad = (act_grad * gate_pre * s).astype(jnp.bfloat16)
        for grad, weight in ((gate_grad, w_gate[i]), (up_grad, w_up[i])):
            term = lax.dot_general(
                grad, weight, (((1,), (1,)), ((), ())), preferred_element_type=jnp.float32
            )
            partial_input = term if partial_input is None else partial_input + term
    input_grad = scatter_sum(partial_input, jnp.float32, jnp.float32, 6)
    return (head_grad, residual_grad, input_grad)


def solution(mesh):
    in_specs = (
        P("expert", None),
        P("expert", None),
        P(),
        P(None, ("expert", "vocab")),
        P("expert"),
        P("expert"),
        P(),
        P("expert", None),
        P("expert", None),
        P("expert", None, "vocab"),
        P("expert", None, "vocab"),
        P("expert", "vocab", None),
    )
    out_specs = (P(None, ("expert", "vocab")), P("expert", "vocab"), P("expert", "vocab"))
    return jax.shard_map(
        on_device, mesh=mesh, in_specs=in_specs, out_specs=out_specs, check_vma=False
    )
```
